32 devices in a mesh: group: 2 (over x), fiber: 16 (over z, y, core).
Axes of the slice: x: 2, y: 2, z: 4, core: 2. Of those that a mesh axis runs over, the one named last changes fastest.
Arguments:
- traces: bfloat16 [1536, 50176], P(('group', 'fiber')), parts along dimension 0, may hold values from -32 to 32
- live_mask: int32 [1536], P(('group', 'fiber')), parts along dimension 0, may hold values from 0 to 1
- source_channels: int32 [4, 8], P('group'), parts along dimension 0, may hold values from 0 to 47
- source_owner: int32 [4], P('group'), parts along dimension 0, may hold values from 0 to 15
Outputs:
- cross_spectra: float32 [2, 8, 1536, 2048], P(None, None, ('group', 'fiber')), parts along dimension 2
The draws below stay inside these ranges and needn't reach their ends.
There are 2 independent parts, one for each index of `group`. The reference program is written for one: setup_inputs(seed, part) draws one part's arguments, and reference() takes and returns one part's arrays. A program takes and returns all parts, laid end to end along the dimension named above; each array names one. Nothing has to cross between parts.
All inputs are finite; a program needn't handle non-finite values.
Results may differ from the reference program's by a relative error of at most 0.00073.
Values may be sent and summed in bfloat16 or wider, within the bound.
No kernel may reach another device: no remote copies, remote signals or barrier semaphores. Data moves between devices by JAX's collectives and lax.ppermute only.
A program may use at most 128 MiB of HBM per device.

```python
import jax
import jax.numpy as jnp
from jax import lax

FRAME = 2048
SMOOTH = 64
RIM = 8
CH_DEV = 48
STEPS = 2
NSRC = 8
SAMPLES = 50176
CHANNELS = 768
N_FIBER = 16


def draw_traces(key, part):
    subkeys = jax.random.split(jax.random.fold_in(key, 11), 6)
    noise_part = jax.random.normal(subkeys[0], (CHANNELS, SAMPLES), jnp.float32)
    channel_scale = jnp.exp(jax.random.uniform(subkeys[2], (CHANNELS,), jnp.float32, jnp.log(0.5), jnp.log(3.0)))
    frequency = jax.random.uniform(subkeys[3], (6,), jnp.float32, 0.02, 0.48)
    sample_time = jnp.arange(SAMPLES, dtype=jnp.float32)
    phase_angle = 2.0 * jnp.pi * jnp.mod(frequency[:, None] * sample_time[None, :], 1.0)
    amplitude = jnp.exp(jax.random.uniform(subkeys[4], (CHANNELS, 6), jnp.float32, jnp.log(0.2), jnp.log(1.2)))
    line_shift = jax.random.uniform(subkeys[5], (CHANNELS, 6), jnp.float32, -jnp.pi, jnp.pi)
    line_part = jnp.dot(amplitude * jnp.cos(line_shift), jnp.sin(phase_angle), precision=lax.Precision.HIGHEST)
    line_part = line_part + jnp.dot(amplitude * jnp.sin(line_shift), jnp.cos(phase_angle), precision=lax.Precision.HIGHEST)
    values = channel_scale[:, None] * (noise_part + line_part)
    return jnp.clip(values, -32.0, 32.0).astype(jnp.bfloat16)


def draw_live_mask(key, part):
    subkeys = jax.random.split(jax.random.fold_in(key, 23), 3)
    isolated = jax.random.randint(subkeys[0], (CHANNELS,), 0, 16) == 0
    run_start = jax.random.randint(subkeys[1], (), 0, CHANNELS - 2 * CH_DEV + 1)
    length = jax.random.randint(subkeys[2], (), CH_DEV // 2, 2 * CH_DEV + 1)
    position = jnp.arange(CHANNELS, dtype=jnp.int32)
    in_run = (position >= run_start) & (position < run_start + length)
    return jnp.where(isolated | in_run, 0, 1).astype(jnp.int32)


def with_ends(entries, key, smallest, high):
    shape = entries.shape
    index_at = [jax.random.randint(jax.random.fold_in(key, axis), (), 0, shape[axis]) for axis in range(len(shape))]
    entries = entries.at[tuple(index_at)].set(smallest)
    longest = shape.index(max(shape))
    index_at[longest] = (index_at[longest] + 1) % shape[longest]
    return entries.at[tuple(index_at)].set(high)


def setup_inputs(seed: int = 0, part: int = 0) -> dict:
    splits = jax.random.split(jax.random.key(seed), 5)
    part_keys = jax.random.split(jax.random.fold_in(splits[4], part), 5)
    traces = draw_traces(jax.random.fold_in(jax.random.fold_in(splits[4], part), 71), part)
    live_mask = draw_live_mask(jax.random.fold_in(jax.random.fold_in(splits[4], part), 71), part)
    source_channels = with_ends(jax.random.randint(part_keys[2], (STEPS, NSRC), 0, CH_DEV), jax.random.fold_in(part_keys[2], 1), 0, CH_DEV - 1).astype(jnp.int32)
    source_owner = jax.random.randint(part_keys[3], (STEPS,), 0, N_FIBER).astype(jnp.int32)
    return dict(traces=traces, live_mask=live_mask, source_channels=source_channels, source_owner=source_owner)


def dft_table(frame_len):
    sample_pos = jnp.arange(frame_len, dtype=jnp.int32)
    bin_pos = jnp.arange(frame_len // 2, dtype=jnp.int32)
    product = sample_pos[:, None] * bin_pos[None, :] % frame_len
    phase_angle = 2.0 * jnp.pi / frame_len * product.astype(jnp.float32)
    hann_window = 0.5 - 0.5 * jnp.cos(2.0 * jnp.pi / frame_len * sample_pos.astype(jnp.float32))
    cosine = hann_window[:, None] * jnp.cos(phase_angle)
    sine = -hann_window[:, None] * jnp.sin(phase_angle)
    return jnp.concatenate([cosine, sine], axis=1).astype(jnp.bfloat16)

def band_matrix(num_bins, half_width):
    bin_pos = jnp.arange(num_bins, dtype=jnp.int32)
    inside = jnp.abs(bin_pos[:, None] - bin_pos[None, :]) <= half_width
    band = inside.astype(jnp.bfloat16)
    bin_count = lax.optimization_barrier(jnp.sum(inside.astype(jnp.float32), axis=0))
    return (band, bin_count)

def spatial_filter(padded, live, rim_width):
    channels = padded.shape[0] - 2 * rim_width
    center = padded[rim_width:rim_width + channels].astype(jnp.float32)
    neighbour_sum = jnp.zeros(center.shape, jnp.float32)
    for offset in range(1, rim_width + 1):
        weight = (rim_width + 1 - offset) / (rim_width * (rim_width + 1.0))
        lower = padded[rim_width - offset:rim_width - offset + channels].astype(jnp.float32)
        upper = padded[rim_width + offset:rim_width + offset + channels].astype(jnp.float32)
        neighbour_sum = neighbour_sum + weight * (lower + upper)
    return (live[:, None] * (center - neighbour_sum)).astype(jnp.bfloat16)

def whiten_rows(filtered, frame_len, half_width):
    rows, samples = filtered.shape
    hop_len = frame_len // 2
    num_frames = samples // hop_len - 1
    num_bins = frame_len // 2
    blocks = filtered.reshape(rows, num_frames + 1, hop_len)
    frames = jnp.concatenate([blocks[:, :-1], blocks[:, 1:]], axis=2).reshape(rows * num_frames, frame_len)
    spectra = jnp.dot(frames, dft_table(frame_len), preferred_element_type=jnp.float32)
    real_part = spectra[:, :num_bins]
    imag_part = spectra[:, num_bins:]
    spectral_power = (real_part * real_part + imag_part * imag_part).astype(jnp.bfloat16)
    band, bin_count = band_matrix(num_bins, half_width)
    smooth = jnp.dot(spectral_power, band, preferred_element_type=jnp.float32) / bin_count[None, :]
    factor = lax.rsqrt(smooth + 1e-06)
    whitened = jnp.concatenate([real_part * factor, imag_part * factor], axis=1).astype(jnp.bfloat16)
    return whitened.reshape(rows, num_frames, frame_len)

def reference(traces, live_mask, source_channels, source_owner):
    channels = traces.shape[0]
    num_bins = FRAME // 2
    premasked = traces * live_mask.astype(jnp.bfloat16)[:, None]
    padded = jnp.concatenate([jnp.zeros((RIM, traces.shape[1]), jnp.bfloat16), premasked, jnp.zeros((RIM, traces.shape[1]), jnp.bfloat16)], axis=0)
    filtered = spatial_filter(padded, live_mask.astype(jnp.float32), RIM)
    whitened = whiten_rows(filtered, FRAME, SMOOTH)
    global_rows = (source_owner[:, None] * CH_DEV + source_channels).astype(jnp.int32)
    sources = whitened[global_rows].astype(jnp.float32)
    whole = whitened.astype(jnp.float32)
    num_frames = whitened.shape[1]
    src_real = sources[..., :num_bins]
    src_imag = sources[..., num_bins:]
    dst_real = whole[..., :num_bins]
    dst_imag = whole[..., num_bins:]
    real_out = jnp.einsum('snfk,cfk->snck', src_real, dst_real) + jnp.einsum('snfk,cfk->snck', src_imag, dst_imag)
    imag_out = jnp.einsum('snfk,cfk->snck', src_real, dst_imag) - jnp.einsum('snfk,cfk->snck', src_imag, dst_real)
    return jnp.concatenate([real_out, imag_out], axis=3) / num_frames
```

```python
import functools

import jax
import jax.numpy as jnp
import numpy as np
from jax import lax
from jax.experimental import pallas as pl
from jax.experimental.pallas import tpu as pltpu
from jax.sharding import PartitionSpec as P

FRAME = 2048
HOP = FRAME // 2
SMOOTH = 64
RIM = 8
STEPS = 2
NSRC = 8
LANES = 128
SCALE = RIM * (RIM + 1)
GROUPS = HOP // (2 * LANES)
VMEM = 48 * 1024 * 1024
BF = jnp.bfloat16
F32 = jnp.float32


def tables():
    n = np.arange(HOP)
    out = []
    for parity in range(2):
        k = 2 * np.arange(HOP // 2) + parity
        ang = 2.0 * np.pi / FRAME * ((n[:, None] * k[None, :]) % FRAME)
        re = np.cos(ang).reshape(HOP, GROUPS, 1, LANES)
        im = -np.sin(ang).reshape(HOP, GROUPS, 1, LANES)
        out.append(np.concatenate([re, im], axis=2).reshape(HOP, HOP))
    k = np.concatenate([np.arange(0, HOP, 2), np.arange(1, HOP, 2)])
    band = (np.abs(k[:, None] - k[None, :]) <= SMOOTH).astype(np.float32)
    icount = (1.0 / band.sum(axis=0))[None, :].astype(np.float32)
    window = (0.5 - 0.5 * np.cos(2.0 * np.pi / FRAME * n))[None, :].astype(np.float32)
    i = np.arange(2 * LANES)
    src = np.where(i % 2 == 0, i // 2, LANES + i // 2)
    weave = (i[:, None] == src[None, :]).astype(np.float32)
    return [
        jnp.asarray(out[0], BF),
        jnp.asarray(out[1], BF),
        jnp.asarray(band, BF),
        jnp.asarray(icount),
        jnp.asarray(window),
        jnp.asarray(weave, BF),
    ]


def tap(distance):
    d = jnp.abs(distance)
    return jnp.where(d == 0, float(SCALE), jnp.where(d <= RIM, (d - RIM - 1).astype(F32), 0.0))


def partial_kernel(pos_ref, base_ref, live_ref, x_ref, out_ref):
    channels = x_ref.shape[0]
    quarter = x_ref.shape[1]
    here = base_ref[0] + lax.broadcasted_iota(jnp.int32, (1, channels), 1)
    dist = pos_ref[...] - here
    live = live_ref[...].astype(F32)
    taps = (tap(dist) * live).astype(BF)
    flag = jnp.sum(jnp.where(dist == 0, live, 0.0), axis=1, keepdims=True)
    part = jnp.dot(taps, x_ref[...], preferred_element_type=F32) * (1.0 / SCALE)
    part = part.astype(BF)
    tail = jnp.broadcast_to(flag, (flag.shape[0], LANES)).astype(BF)
    for step in range(STEPS):
        rows = slice(step * NSRC, (step + 1) * NSRC)
        out_ref[step, 0, :, :quarter] = part[rows]
        out_ref[step, 0, :, quarter:] = tail[rows]


def partial_sources(traces, live, pos, base):
    channels, samples = traces.shape
    quarter = samples // 4
    return pl.pallas_call(
        partial_kernel,
        name="partial_sources",
        grid=(4,),
        in_specs=[
            pl.BlockSpec(pos.shape, lambda q: (0, 0)),
            pl.BlockSpec(memory_space=pltpu.SMEM),
            pl.BlockSpec((1, channels), lambda q: (0, 0)),
            pl.BlockSpec((channels, quarter), lambda q: (0, q)),
        ],
        out_specs=pl.BlockSpec((STEPS, 1, NSRC, quarter + LANES), lambda q: (0, q, 0, 0)),
        out_shape=jax.ShapeDtypeStruct((STEPS, 4, NSRC, quarter + LANES), BF),
        compiler_params=pltpu.CompilerParams(vmem_limit_bytes=VMEM),
    )(pos, base, live, traces)


def whiten_block(u_ref, v_ref, y_ref, te, to, band, icount, store, rows, block):
    y_ref[0] = jnp.dot(u_ref[...], te, preferred_element_type=F32)
    y_ref[1] = jnp.dot(v_ref[...], to, preferred_element_type=F32)

    def power(i, carry):
        r = pl.ds(pl.multiple_of(i * block, block), block)
        for parity, ref in ((0, u_ref), (1, v_ref)):
            for g in range(GROUPS):
                re = y_ref[parity, r, 2 * g * LANES : (2 * g + 1) * LANES]
                im = y_ref[parity, r, (2 * g + 1) * LANES : (2 * g + 2) * LANES]
                lo = (parity * GROUPS + g) * LANES
                u_ref[r, lo : lo + LANES] = (re * re + im * im).astype(BF)
        return carry

    lax.fori_loop(0, rows // block, power, 0)
    smooth = jnp.dot(u_ref[...], band, preferred_element_type=F32)
    y_ref[2] = smooth

    def scale(i, carry):
        r = pl.ds(pl.multiple_of(i * block, block), block)
        for parity in range(2):
            for g in range(GROUPS):
                lo = (parity * GROUPS + g) * LANES
                factor = lax.rsqrt(y_ref[2, r, lo : lo + LANES] * icount[:, lo : lo + LANES] + 1e-06)
                re = y_ref[parity, r, 2 * g * LANES : (2 * g + 1) * LANES]
                im = y_ref[parity, r, (2 * g + 1) * LANES : (2 * g + 2) * LANES]
                both = jnp.concatenate([re * factor, im * factor], axis=1)
                store(i, g * 4 * LANES + parity * 2 * LANES, both)
        return carry

    lax.fori_loop(0, rows // block, scale, 0)


def own_kernel(a_ref, x_ref, nxt_ref, te_ref, to_ref, band_ref, ic_ref, w_ref, out_ref, u_ref, v_ref, y_ref):
    frames = x_ref.shape[1] // HOP
    rows = a_ref.shape[0]
    a = a_ref[...]
    w = w_ref[...]

    def filt(block):
        full = jnp.dot(a, block, preferred_element_type=F32) * (1.0 / SCALE)
        return full.astype(BF).astype(F32)

    b = filt(x_ref[:, :HOP])
    early = b * w
    for f in range(frames):
        nb = filt(x_ref[:, (f + 1) * HOP : (f + 2) * HOP] if f + 1 < frames else nxt_ref[...])
        nearly = nb * w
        late = nb - nearly
        u_ref[f * rows : (f + 1) * rows] = (early + late).astype(BF)
        v_ref[f * rows : (f + 1) * rows] = (early - late).astype(BF)
        early = nearly

    def store(i, lo, both):
        out_ref[i, :, lo : lo + 2 * LANES] = both.astype(BF)

    whiten_block(u_ref, v_ref, y_ref, te_ref[...], to_ref[...], band_ref[...], ic_ref[...], store, frames * rows, rows)


def whiten_own(x, a, tabs, per):
    te, to, band, icount, window, _ = tabs
    rows_in, samples = x.shape
    rows = a.shape[0]
    frames = samples // HOP - 1
    const = lambda j: (0, 0)
    return pl.pallas_call(
        own_kernel,
        name="whiten_own",
        grid=(frames // per,),
        in_specs=[
            pl.BlockSpec(a.shape, const),
            pl.BlockSpec((rows_in, per * HOP), lambda j: (0, j)),
            pl.BlockSpec((rows_in, HOP), lambda j: (0, (j + 1) * per)),
            pl.BlockSpec(te.shape, const),
            pl.BlockSpec(to.shape, const),
            pl.BlockSpec(band.shape, const),
            pl.BlockSpec(icount.shape, const),
            pl.BlockSpec(window.shape, const),
        ],
        out_specs=pl.BlockSpec((per, rows, FRAME), lambda j: (j, 0, 0)),
        out_shape=jax.ShapeDtypeStruct((frames, rows, FRAME), BF),
        scratch_shapes=[
            pltpu.VMEM((per * rows, HOP), BF),
            pltpu.VMEM((per * rows, HOP), BF),
            pltpu.VMEM((3, per * rows, HOP), F32),
        ],
        compiler_params=pltpu.CompilerParams(vmem_limit_bytes=VMEM),
    )(a, x, x, te, to, band, icount, window)


def source_kernel(half_ref, mine_ref, other_ref, te_ref, to_ref, band_ref, ic_ref, w_ref, out_ref, x_ref, u_ref, v_ref, y_ref):
    quarter = mine_ref.shape[2] - LANES
    rows = mine_ref.shape[1]
    frames = out_ref.shape[0]

    def place(first, second):
        for i, ref in ((0, first), (1, second)):
            for q in range(2):
                x_ref[:, (2 * i + q) * quarter : (2 * i + q + 1) * quarter] = ref[q, :, :quarter]

    @pl.when(half_ref[0] == 0)
    def _():
        place(mine_ref, other_ref)

    @pl.when(half_ref[0] != 0)
    def _():
        place(other_ref, mine_ref)

    flag = mine_ref[0, :, quarter:].astype(F32)[:, :1]
    w = w_ref[...]
    b = x_ref[:, :HOP].astype(F32) * flag
    early = b * w
    for f in range(0, frames, 2):
        us = []
        vs = []
        for g in (f, f + 1):
            nb = x_ref[:, (g + 1) * HOP : (g + 2) * HOP].astype(F32) * flag
            nearly = nb * w
            late = nb - nearly
            us.append(early + late)
            vs.append(early - late)
            early = nearly
        u_ref[f * rows : (f + 2) * rows] = jnp.concatenate(us, axis=0).astype(BF)
        v_ref[f * rows : (f + 2) * rows] = jnp.concatenate(vs, axis=0).astype(BF)

    def store(i, lo, both):
        out_ref[2 * i, :, lo : lo + 2 * LANES] = both[:rows].astype(BF)
        out_ref[2 * i + 1, :, lo : lo + 2 * LANES] = both[rows:].astype(BF)

    whiten_block(u_ref, v_ref, y_ref, te_ref[...], to_ref[...], band_ref[...], ic_ref[...], store, frames * rows, 2 * rows)


def whiten_source(half, mine, other, tabs):
    te, to, band, icount, window, _ = tabs
    samples = 4 * (mine.shape[2] - LANES)
    rows = mine.shape[1]
    frames = samples // HOP - 1
    return pl.pallas_call(
        source_kernel,
        name="whiten_source",
        in_specs=[pl.BlockSpec(memory_space=pltpu.SMEM)] + [pl.BlockSpec(memory_space=pltpu.VMEM)] * 7,
        out_specs=pl.BlockSpec(memory_space=pltpu.VMEM),
        out_shape=jax.ShapeDtypeStruct((frames, rows, FRAME), BF),
        scratch_shapes=[
            pltpu.VMEM((rows, samples), BF),
            pltpu.VMEM((frames * rows, HOP), BF),
            pltpu.VMEM((frames * rows, HOP), BF),
            pltpu.VMEM((3, frames * rows, HOP), F32),
        ],
        compiler_params=pltpu.CompilerParams(vmem_limit_bytes=VMEM),
    )(half, mine, other, te, to, band, icount, window)


SGRP = 4


def cross_kernel(src_ref, mid_ref, edge_ref, weave_ref, *rest):
    out_ref, s_ref, e_ref, im_ref = rest[-4:]
    frames, nsrc = src_ref.shape[:2]
    mid = mid_ref.shape[1]
    edge = edge_ref.shape[1]
    weave = weave_ref[...]

    def product(ref, c0, parity, s0):
        lo = parity * 2 * LANES

        def body(f, acc):
            wr = ref[f, c0 : c0 + 16, lo : lo + LANES].astype(F32)
            wi = ref[f, c0 : c0 + 16, lo + LANES : lo + 2 * LANES].astype(F32)
            ws = wr + wi
            wd = wi - wr
            new = []
            for j in range(SGRP):
                s = s0 + j
                sr = s_ref[f, s : s + 1, lo : lo + LANES]
                si = s_ref[f, s : s + 1, lo + LANES : lo + 2 * LANES]
                ss = s_ref[f, s : s + 1, 4 * LANES + parity * LANES : 4 * LANES + (parity + 1) * LANES]
                a, b, c = acc[j]
                new.append((a + sr * ws, b + ss * wr, c + si * wd))
            return tuple(new)

        zero = jnp.zeros((16, LANES), F32)
        acc = lax.fori_loop(0, frames, body, tuple((zero, zero, zero) for _ in range(SGRP)), unroll=2)
        return [((b + c) * (1.0 / frames), (a - b) * (1.0 / frames)) for a, b, c in acc]

    @pl.when(pl.program_id(1) == 0)
    def _():
        for parity in range(2):
            lo = parity * 2 * LANES
            both = src_ref[:, :, lo : lo + 2 * LANES].astype(F32)
            s_ref[:, :, lo : lo + 2 * LANES] = both
            s_ref[:, :, 4 * LANES + parity * LANES : 4 * LANES + (parity + 1) * LANES] = (
                both[:, :, :LANES] + both[:, :, LANES:]
            )
        rim = edge // 2
        for ref, c0, spots in [(mid_ref, c, ((rim + c, 0, 16),)) for c in range(0, mid, 16)] + [
            (edge_ref, 0, ((0, 0, rim), (rim + mid, rim, 2 * rim)))
        ]:
            for s0 in range(0, nsrc, SGRP):
                halves = [product(ref, c0, parity, s0) for parity in range(2)]
                for j in range(SGRP):
                    for part in range(2):
                        both = jnp.concatenate([halves[0][j][part], halves[1][j][part]], axis=1)
                        for d0, a, b in spots:
                            e_ref[part, s0 + j, d0 : d0 + b - a, :] = both[a:b]

        for part in range(2):
            full = e_ref[part].reshape(nsrc * (mid + edge), 2 * LANES)
            hi = full.astype(BF)
            lo = (full - hi.astype(F32)).astype(BF)
            res = jnp.dot(hi, weave, preferred_element_type=F32) + jnp.dot(lo, weave, preferred_element_type=F32)
            res = res.reshape(nsrc, mid + edge, 2 * LANES)
            if part == 0:
                out_ref[0] = res
            else:
                im_ref[...] = res

    @pl.when(pl.program_id(1) != 0)
    def _():
        out_ref[0] = im_ref[...]


def cross(src, mid, edge, weave, step, previous):
    frames, nsrc, _ = src.shape
    channels = mid.shape[1] + edge.shape[1]
    width = 4 * LANES
    shape = jax.ShapeDtypeStruct((STEPS, nsrc, channels, FRAME), F32)
    args = [src, mid, edge, weave]
    specs = [pl.BlockSpec((frames, a.shape[1], width), lambda g, p: (0, 0, g)) for a in args[:3]]
    specs.append(pl.BlockSpec(weave.shape, lambda g, p: (0, 0)))
    alias = {}
    if previous is not None:
        args.append(previous)
        specs.append(pl.BlockSpec(memory_space=pl.ANY))
        alias = {4: 0}
    return pl.pallas_call(
        cross_kernel,
        name="cross",
        grid=(GROUPS, 2),
        in_specs=specs,
        out_specs=pl.BlockSpec((1, nsrc, channels, 2 * LANES), lambda g, p: (step, 0, 0, p * GROUPS + g)),
        out_shape=shape,
        scratch_shapes=[
            pltpu.VMEM((frames, nsrc, 6 * LANES), F32),
            pltpu.VMEM((2, nsrc, channels, 2 * LANES), F32),
            pltpu.VMEM((nsrc, channels, 2 * LANES), F32),
        ],
        input_output_aliases=alias,
        compiler_params=pltpu.CompilerParams(vmem_limit_bytes=VMEM),
    )(*args)


def swap(block, bit, count):
    return lax.ppermute(block, "fiber", [(i, i ^ bit) for i in range(count)])


def fiber_halves(part):
    count = lax.axis_size("fiber")
    me = lax.axis_index("fiber")
    c = me & 1
    y = (me >> 1) & 1
    give = lax.dynamic_slice_in_dim(part, 2 * (1 - c), 2, axis=0)
    keep = lax.dynamic_slice_in_dim(part, 2 * c, 2, axis=0)
    half = keep + swap(give, 1, count)
    give = lax.dynamic_slice_in_dim(half, 1 - y, 1, axis=0)
    keep = lax.dynamic_slice_in_dim(half, y, 1, axis=0)
    piece = keep + swap(give, 2, count)
    bit = 4
    while bit < count:
        piece = piece + swap(piece, bit, count)
        bit *= 2
    twin = swap(piece, 2, count)
    mine = jnp.where(y == 0, jnp.concatenate([piece, twin]), jnp.concatenate([twin, piece]))
    return mine, swap(mine, 1, count)


def on_device(traces, live_mask, source_channels, source_owner):
    tabs = tables()
    channels = traces.shape[0]
    count = lax.axis_size("fiber")
    me = lax.axis_index("fiber")
    live_f = live_mask.astype(F32)

    pos = (source_owner[:, None] * channels + source_channels).reshape(STEPS * NSRC, 1)
    base = (me * channels).reshape(1)
    part = partial_sources(traces, live_mask.reshape(1, channels), pos, base)

    live_b = live_mask.astype(BF)[:, None]
    forward = [(i, i + 1) for i in range(count - 1)]
    backward = [(i + 1, i) for i in range(count - 1)]

    gathered = [fiber_halves(part[step]) for step in range(STEPS)]

    low = lax.ppermute(traces[channels - RIM :] * live_b[channels - RIM :], "fiber", forward)
    high = lax.ppermute(traces[:RIM] * live_b[:RIM], "fiber", backward)

    idx = jnp.arange(channels)
    mid_idx = idx[RIM : channels - RIM]
    a_mid = tap(mid_idx[:, None] - idx[None, :]) * live_f[mid_idx][:, None] * live_f[None, :]
    edge_in = jnp.concatenate([low, traces[: 2 * RIM], traces[channels - 2 * RIM :], high], axis=0)
    in_pos = np.concatenate([np.arange(-RIM, 2 * RIM), np.arange(channels - 2 * RIM, channels + RIM)])
    out_pos = np.concatenate([np.arange(RIM), np.arange(channels - RIM, channels)])
    in_live = jnp.concatenate(
        [jnp.ones((RIM,), F32), live_f[: 2 * RIM], live_f[channels - 2 * RIM :], jnp.ones((RIM,), F32)]
    )
    near = (in_pos[None, :] < channels // 2) == (out_pos[:, None] < channels // 2)
    a_edge = jnp.where(near, tap(jnp.asarray(out_pos[:, None] - in_pos[None, :])), 0.0)
    a_edge = a_edge * live_f[out_pos][:, None] * in_live[None, :]

    mid = whiten_own(traces, a_mid.astype(BF), tabs, 8)
    edge = whiten_own(edge_in, a_edge.astype(BF), tabs, 16)

    half = (me & 1).reshape(1)
    out = None
    for step in range(STEPS):
        mine, other = gathered[step]
        src = whiten_source(half, mine, other, tabs)
        out = cross(src, mid, edge, tabs[5], step, out)
    return out


def solution(mesh):
    placed = (P(("group", "fiber"), None), P(("group", "fiber")), P("group", None), P("group"))
    return jax.shard_map(
        on_device,
        mesh=mesh,
        in_specs=placed,
        out_specs=P(None, None, ("group", "fiber"), None),
        check_vma=False,
    )
```

```python
import functools

import jax
import jax.numpy as jnp
import numpy as np
from jax import lax
from jax.experimental import pallas as pl
from jax.experimental.pallas import tpu as pltpu
from jax.sharding import PartitionSpec as P

FRAME = 2048
HOP = FRAME // 2
SMOOTH = 64
RIM = 8
STEPS = 2
NSRC = 8
LANES = 128
SCALE = RIM * (RIM + 1)
GROUPS = HOP // (2 * LANES)
VMEM = 14 * 1024 * 1024
SPLIT = 2
PIECES = 3
BF = jnp.bfloat16
F32 = jnp.float32


def tables():
    n = np.arange(HOP)
    out = []
    for parity in range(2):
        k = 2 * np.arange(HOP // 2) + parity
        ang = 2.0 * np.pi / FRAME * ((n[:, None] * k[None, :]) % FRAME)
        re = np.cos(ang).reshape(HOP, GROUPS, 1, LANES)
        im = -np.sin(ang).reshape(HOP, GROUPS, 1, LANES)
        out.append(np.concatenate([re, im], axis=2).reshape(HOP, HOP))
    k = np.concatenate([np.arange(0, HOP, 2), np.arange(1, HOP, 2)])
    band = (np.abs(k[:, None] - k[None, :]) <= SMOOTH).astype(np.float32)
    icount = (1.0 / band.sum(axis=0))[None, :].astype(np.float32)
    window = (0.5 - 0.5 * np.cos(2.0 * np.pi / FRAME * n))[None, :].astype(np.float32)
    i = np.arange(2 * LANES)
    src = np.where(i % 2 == 0, i // 2, LANES + i // 2)
    weave = (i[:, None] == src[None, :]).astype(np.float32)
    return [
        jnp.asarray(out[0], BF),
        jnp.asarray(out[1], BF),
        jnp.asarray(band, BF),
        jnp.asarray(icount),
        jnp.asarray(window),
        jnp.asarray(weave, BF),
    ]


def tap(distance):
    d = jnp.abs(distance)
    return jnp.where(d == 0, float(SCALE), jnp.where(d <= RIM, (d - RIM - 1).astype(F32), 0.0))


def partial_kernel(me_ref, pos_ref, live_ref, x_ref, give_ref, keep_ref, low_ref, high_ref):
    channels, quarter = x_ref.shape
    here = me_ref[0] * channels + lax.broadcasted_iota(jnp.int32, (1, channels), 1)
    dist = pos_ref[...] - here
    live = live_ref[:1, :channels]
    taps = (tap(dist) * live).astype(BF)
    flag = jnp.sum(jnp.where(dist == 0, live, 0.0), axis=1, keepdims=True)
    part = jnp.dot(taps, x_ref[...], preferred_element_type=F32) * (1.0 / SCALE)
    part = part.astype(BF)
    tail = jnp.broadcast_to(flag, (flag.shape[0], LANES)).astype(BF)

    def put(ref):
        for step in range(STEPS):
            rows = slice(step * NSRC, (step + 1) * NSRC)
            ref[step, 0, :, :quarter] = part[rows]
            ref[step, 0, :, quarter:] = tail[rows]

    @pl.when(pl.program_id(0) < 2)
    def _():
        put(give_ref)

    @pl.when(pl.program_id(0) >= 2)
    def _():
        put(keep_ref)

    shape = (channels, channels)
    diagonal = lax.broadcasted_iota(jnp.int32, shape, 0) == lax.broadcasted_iota(jnp.int32, shape, 1)
    livec = jnp.sum(jnp.where(diagonal, live, 0.0), axis=1, keepdims=True)
    low_ref[...] = (x_ref[:RIM].astype(F32) * livec[:RIM]).astype(BF)
    high_ref[...] = (x_ref[channels - RIM :].astype(F32) * livec[channels - RIM :]).astype(BF)


def partial_sources(traces, live, pos, me):
    channels, samples = traces.shape
    quarter = samples // 4

    def place(i, me_ref):
        c = me_ref[0] & 1
        y = (me_ref[0] >> SPLIT) & 1
        half = jnp.where(i < 2, 1 - c, c)
        return 2 * half + jnp.where(i % 2 == 0, 1 - y, y)

    const = lambda i, me_ref: (0, 0)
    slab = jax.ShapeDtypeStruct((STEPS, 2, NSRC, quarter + LANES), BF)
    rim = jax.ShapeDtypeStruct((RIM, samples), BF)
    rim_spec = pl.BlockSpec((RIM, quarter), lambda i, me_ref: (0, place(i, me_ref)))
    return pl.pallas_call(
        partial_kernel,
        name="partial_sources",
        grid_spec=pltpu.PrefetchScalarGridSpec(
            num_scalar_prefetch=1,
            grid=(4,),
            in_specs=[
                pl.BlockSpec(pos.shape, const),
                pl.BlockSpec(live.shape, const),
                pl.BlockSpec((channels, quarter), lambda i, me_ref: (0, place(i, me_ref))),
            ],
            out_specs=[
                pl.BlockSpec((STEPS, 1, NSRC, quarter + LANES), lambda i, me_ref: (0, jnp.minimum(i, 1), 0, 0)),
                pl.BlockSpec((STEPS, 1, NSRC, quarter + LANES), lambda i, me_ref: (0, jnp.maximum(i - 2, 0), 0, 0)),
                rim_spec,
                rim_spec,
            ],
        ),
        out_shape=[slab, slab, rim, rim],
        compiler_params=pltpu.CompilerParams(vmem_limit_bytes=VMEM),
    )(me, pos, live, traces)


TABLE = pl.BlockSpec(memory_space=pltpu.VMEM)


def whiten_block(u, v, te_ref, to_ref, band_ref, ic_ref, store):
    y = [
        jnp.dot(u, te_ref[...], preferred_element_type=F32),
        jnp.dot(v, to_ref[...], preferred_element_type=F32),
    ]
    half = HOP // 2
    smooth = None
    for parity in range(2):
        power = []
        for g in range(GROUPS):
            re = y[parity][:, 2 * g * LANES : (2 * g + 1) * LANES]
            im = y[parity][:, (2 * g + 1) * LANES : (2 * g + 2) * LANES]
            power.append((re * re + im * im).astype(BF))
        power = jnp.concatenate(power, axis=1)
        part = jnp.dot(power, band_ref[parity * half : (parity + 1) * half], preferred_element_type=F32)
        smooth = part if smooth is None else smooth + part
    for parity in range(2):
        for g in range(GROUPS):
            lo = (parity * GROUPS + g) * LANES
            factor = lax.rsqrt(smooth[:, lo : lo + LANES] * ic_ref[:, lo : lo + LANES] + 1e-06)
            re = y[parity][:, 2 * g * LANES : (2 * g + 1) * LANES]
            im = y[parity][:, (2 * g + 1) * LANES : (2 * g + 2) * LANES]
            store(g, parity, *((x * factor).astype(BF).astype(F32) for x in (re, im)))


def own_kernel(pieces, channels, rows, live_ref, *refs):
    xs = refs[: 2 * pieces]
    te_ref, to_ref, band_ref, ic_ref, w_ref, out_ref, u_ref, v_ref = refs[2 * pieces :]
    frames = xs[0].shape[1] // HOP
    w = w_ref[...]
    width = sum(r.shape[0] for r in xs[:pieces])
    o = lax.broadcasted_iota(jnp.int32, (rows, 1), 0)
    i = lax.broadcasted_iota(jnp.int32, (1, width), 1)
    if pieces == 1:
        o = o + RIM
        live = live_ref[:1, :width]
    else:
        tail = channels - 2 * RIM
        o = jnp.where(o < RIM, o, o + tail)
        both = live_ref[...]
        lane = lax.broadcasted_iota(jnp.int32, both.shape, 1)
        back = pltpu.roll(both, LANES - tail + 2 * RIM, 1)
        both = jnp.where(lane < 2 * RIM, both, jnp.where(lane < 4 * RIM, back, 1.0))
        live = both[:1, :width]
        far = jnp.where(i < 5 * RIM, i - 5 * RIM, i - 5 * RIM + channels)
        i = jnp.where(i < 2 * RIM, i, jnp.where(i < 4 * RIM, i + tail - 2 * RIM, far))
    keep = jnp.sum(jnp.where(o == i, live, 0.0), axis=1, keepdims=True)
    a = (tap(o - i) * live * keep).astype(BF)

    def filt(f):
        if f < frames:
            parts = [r[:, f * HOP : (f + 1) * HOP] for r in xs[:pieces]]
        else:
            parts = [r[...] for r in xs[pieces:]]
        block = parts[0] if pieces == 1 else jnp.concatenate(parts, axis=0)
        full = jnp.dot(a, block, preferred_element_type=F32) * (1.0 / SCALE)
        return full.astype(BF).astype(F32)

    b = filt(0)
    early = b * w
    for f in range(frames):
        nb = filt(f + 1)
        nearly = nb * w
        late = nb - nearly
        u_ref[f * rows : (f + 1) * rows] = (early + late).astype(BF)
        v_ref[f * rows : (f + 1) * rows] = (early - late).astype(BF)
        early = nearly

    def store(g, parity, re, im):
        at = (2 * g + parity) * 3 * LANES
        for i, value in enumerate((re, re + im, im - re)):
            out_ref[:, :, at + i * LANES : at + (i + 1) * LANES] = value.reshape(frames, rows, LANES)

    whiten_block(u_ref[...], v_ref[...], te_ref, to_ref, band_ref, ic_ref, store)


def whiten_own(xs, live, rows, channels, tabs, per, first, frames):
    te, to, band, icount, window, _ = tabs
    j0 = first // per
    specs = [pl.BlockSpec((size, per * HOP), lambda j, b=at: (b, j0 + j)) for _, size, at in xs]
    specs += [pl.BlockSpec((size, HOP), lambda j, b=at: (b, (j0 + j + 1) * per)) for _, size, at in xs]
    return pl.pallas_call(
        functools.partial(own_kernel, len(xs), channels, rows),
        grid=(frames // per,),
        in_specs=[pl.BlockSpec(live.shape, lambda j: (0, 0))] + specs + [TABLE] * 5,
        out_specs=pl.BlockSpec((per, rows, 3 * HOP), lambda j: (j, 0, 0)),
        out_shape=jax.ShapeDtypeStruct((frames, rows, 3 * HOP), F32),
        scratch_shapes=[pltpu.VMEM((per * rows, HOP), BF), pltpu.VMEM((per * rows, HOP), BF)],
        compiler_params=pltpu.CompilerParams(vmem_limit_bytes=VMEM),
    )(live, *[x[0] for x in xs], *[x[0] for x in xs], te, to, band, icount, window)


def source_kernel(me_ref, mine_ref, twin_ref, pair_ref, far_ref, te_ref, to_ref, band_ref, ic_ref, w_ref, out_ref, x_ref, u_ref, v_ref):
    quarter = mine_ref.shape[2] - LANES
    rows = mine_ref.shape[1]
    frames = out_ref.shape[0]
    q = (me_ref[0] & 1) * 2 + ((me_ref[0] >> SPLIT) & 1)
    for at in range(4):

        @pl.when(q == at)
        def _(at=at):
            for flip, ref in ((0, mine_ref), (1, twin_ref), (2, pair_ref), (3, far_ref)):
                to = at ^ flip
                x_ref[:, to * quarter : (to + 1) * quarter] = ref[0, :, :quarter]

    flag = mine_ref[0, :, quarter:].astype(F32)[:, :1]
    w = w_ref[...]
    b = x_ref[:, :HOP].astype(F32) * flag
    early = b * w
    for f in range(0, frames, 2):
        us = []
        vs = []
        for g in (f, f + 1):
            nb = x_ref[:, (g + 1) * HOP : (g + 2) * HOP].astype(F32) * flag
            nearly = nb * w
            late = nb - nearly
            us.append(early + late)
            vs.append(early - late)
            early = nearly
        u_ref[f * rows : (f + 2) * rows] = jnp.concatenate(us, axis=0).astype(BF)
        v_ref[f * rows : (f + 2) * rows] = jnp.concatenate(vs, axis=0).astype(BF)

    def store(g, parity, re, im):
        at = (2 * g + parity) * 3 * LANES
        for i, value in enumerate((re, im, re + im)):
            out_ref[:, :, at + i * LANES : at + (i + 1) * LANES] = value.reshape(frames, rows, LANES)

    whiten_block(u_ref[...], v_ref[...], te_ref, to_ref, band_ref, ic_ref, store)


def whiten_source(me, quarters, tabs):
    te, to, band, icount, window, _ = tabs
    samples = 4 * (quarters[0].shape[2] - LANES)
    rows = quarters[0].shape[1]
    frames = samples // HOP - 1
    return pl.pallas_call(
        source_kernel,
        name="whiten_source",
        in_specs=[pl.BlockSpec(memory_space=pltpu.SMEM)] + [TABLE] * 9,
        out_specs=TABLE,
        out_shape=jax.ShapeDtypeStruct((frames, rows, 3 * HOP), F32),
        scratch_shapes=[
            pltpu.VMEM((rows, samples), BF),
            pltpu.VMEM((frames * rows, HOP), BF),
            pltpu.VMEM((frames * rows, HOP), BF),
        ],
        compiler_params=pltpu.CompilerParams(vmem_limit_bytes=VMEM),
    )(me, *quarters, te, to, band, icount, window)


SGRP = 4
UNROLL = 16


def cross_kernel(count, group, src_ref, *rest):
    mids = rest[:count]
    edges = rest[count : 2 * count]
    weave_ref = rest[2 * count]
    out_ref, e_ref, im_ref = rest[-3:]
    frames, nsrc = src_ref.shape[:2]
    mid = mids[0].shape[1]
    edge = edges[0].shape[1]
    weave = weave_ref[...]

    def product(refs, c0, parity, s0):
        lo = (2 * group + parity) * 3 * LANES
        zero = jnp.zeros((16, LANES), F32)
        acc = tuple((zero, zero, zero) for _ in range(SGRP))
        start = 0
        for ref in refs:

            def body(f, acc, ref=ref, start=start):
                wr, ws, wd = (ref[f, c0 : c0 + 16, lo + i * LANES : lo + (i + 1) * LANES] for i in range(3))
                new = []
                for j in range(SGRP):
                    s = slice(s0 + j, s0 + j + 1)
                    sr, si, ss = (
                        src_ref[start + f, s, lo + i * LANES : lo + (i + 1) * LANES] for i in range(3)
                    )
                    a, b, c = acc[j]
                    new.append((a + sr * ws, b + ss * wr, c + si * wd))
                return tuple(new)

            acc = lax.fori_loop(0, ref.shape[0], body, acc, unroll=UNROLL)
            start += ref.shape[0]
        return [((b + c) * (1.0 / frames), (a - b) * (1.0 / frames)) for a, b, c in acc]

    @pl.when(pl.program_id(0) == 0)
    def _():
        rim = edge // 2
        for refs, c0, spots in [(mids, c, ((rim + c, 0, 16),)) for c in range(0, mid, 16)] + [
            (edges, 0, ((0, 0, rim), (rim + mid, rim, 2 * rim)))
        ]:
            for s0 in range(0, nsrc, SGRP):
                halves = [product(refs, c0, parity, s0) for parity in range(2)]
                for j in range(SGRP):
                    for part in range(2):
                        both = jnp.concatenate([halves[0][j][part], halves[1][j][part]], axis=1)
                        for d0, a, b in spots:
                            e_ref[part, s0 + j, d0 : d0 + b - a, :] = both[a:b]

        for part in range(2):
            full = e_ref[part].reshape(nsrc * (mid + edge), 2 * LANES)
            hi = full.astype(BF)
            lo = (full - hi.astype(F32)).astype(BF)
            res = jnp.dot(hi, weave, preferred_element_type=F32) + jnp.dot(lo, weave, preferred_element_type=F32)
            res = res.reshape(nsrc, mid + edge, 2 * LANES)
            if part == 0:
                out_ref[0] = res
            else:
                im_ref[...] = res

    @pl.when(pl.program_id(0) != 0)
    def _():
        out_ref[0] = im_ref[...]


def cross(src, mids, edges, weave, step, group, previous):
    _, nsrc, _ = src.shape
    channels = mids[0].shape[1] + edges[0].shape[1]
    shape = jax.ShapeDtypeStruct((STEPS, nsrc, channels, FRAME), F32)
    args = [src, *mids, *edges, weave]
    specs = [TABLE] * len(args)
    alias = {}
    if previous is not None:
        alias = {len(args): 0}
        args.append(previous)
        specs.append(pl.BlockSpec(memory_space=pl.ANY))
    return pl.pallas_call(
        functools.partial(cross_kernel, len(mids), group),
        name="cross",
        grid=(2,),
        in_specs=specs,
        out_specs=pl.BlockSpec((1, nsrc, channels, 2 * LANES), lambda p: (step, 0, 0, p * GROUPS + group)),
        out_shape=shape,
        scratch_shapes=[
            pltpu.VMEM((2, nsrc, channels, 2 * LANES), F32),
            pltpu.VMEM((nsrc, channels, 2 * LANES), F32),
        ],
        input_output_aliases=alias,
        compiler_params=pltpu.CompilerParams(vmem_limit_bytes=VMEM),
    )(*args)


def swap(block, bit):
    return lax.ppermute(block, "fiber", [(i, i ^ bit) for i in range(lax.axis_size("fiber"))])


def after(x, *deps):
    return lax.optimization_barrier((x, deps))[0]


def on_device(traces, live_mask, source_channels, source_owner):
    tabs = tables()
    channels, samples = traces.shape
    frames = samples // HOP - 1
    count = lax.axis_size("fiber")
    me = lax.axis_index("fiber").reshape(1)
    live = jnp.broadcast_to(jnp.pad(live_mask.astype(F32), (0, LANES - channels)), (8, LANES))

    pos = (source_owner[:, None] * channels + source_channels).reshape(STEPS * NSRC, 1)
    give, keep, low, high = partial_sources(traces, live, pos, me)

    span = frames // PIECES

    def mid(p, *deps):
        xs = [(traces, channels, 0)]
        return whiten_own(xs, after(live, *deps), channels - 2 * RIM, channels, tabs, 8, p * span, span)

    last = channels // (2 * RIM) - 1

    def edge(p, low, high, *deps):
        xs = [(traces, 2 * RIM, 0), (traces, 2 * RIM, last), (low, RIM, 0), (high, RIM, 0)]
        return whiten_own(xs, after(live, *deps), 2 * RIM, channels, tabs, 16, p * span, span)

    others = [1 << b for b in range(count.bit_length() - 2, 0, -1) if b != SPLIT]

    first = [swap(give[step], 1) for step in range(STEPS)]
    half_a = keep[0] + first[0]
    move = swap(half_a[:1], 1 << SPLIT)
    low_to, high_to = after((low, high), half_a)
    low = lax.ppermute(high_to, "fiber", [(i, i + 1) for i in range(count - 1)])
    high = lax.ppermute(low_to, "fiber", [(i + 1, i) for i in range(count - 1)])
    mids = [mid(0, half_a)]
    piece_a = half_a[1:] + after(move, mids[0])
    move = swap(piece_a, others[0])
    half_b = keep[1] + after(first[1], piece_a)
    move_b = swap(half_b[:1], 1 << SPLIT)
    mids.append(mid(1, piece_a, half_b))
    mids.append(mid(2, mids[1]))
    piece_b = half_b[1:] + after(move_b, mids[2])
    for bit in others[1:]:
        piece_a = piece_a + after(move, mids[2])
        move = swap(piece_a, bit)
    move_b = swap(piece_b, others[0])
    edges = [edge(0, low, high, piece_a, piece_b)]
    edges.append(edge(1, low, high, edges[0]))
    piece_a = piece_a + after(move, edges[1])
    twin_a = swap(piece_a, 1 << SPLIT)
    pair_a = swap(piece_a, 1)
    edges.append(edge(2, low, high, piece_a))
    for bit in others[1:]:
        piece_b = piece_b + after(move_b, edges[2])
        move_b = swap(piece_b, bit)
    far_a = swap(after(twin_a, edges[2]), 1)
    src = whiten_source(me, (piece_a, twin_a, pair_a, far_a), tabs)
    out = cross(src, mids, edges, tabs[5], 0, 0, None)
    piece_b = piece_b + after(move_b, out)
    twin_b = swap(piece_b, 1 << SPLIT)
    pair_b = swap(piece_b, 1)
    out = cross(after(src, piece_b), mids, edges, tabs[5], 0, 1, out)
    far_b = swap(after(twin_b, out), 1)
    for g in range(2, GROUPS):
        out = cross(after(src, out, twin_b), mids, edges, tabs[5], 0, g, out)
    src = whiten_source(me, (piece_b, twin_b, pair_b, after(far_b, out)), tabs)
    for g in range(GROUPS):
        out = cross(src, mids, edges, tabs[5], 1, g, out)
    return out


def solution(mesh):
    placed = (P(("group", "fiber"), None), P(("group", "fiber")), P("group", None), P("group"))
    return jax.shard_map(
        on_device,
        mesh=mesh,
        in_specs=placed,
        out_specs=P(None, None, ("group", "fiber"), None),
        check_vma=False,
    )
```

```python
import functools

import jax
import jax.numpy as jnp
import numpy as np
from jax import lax
from jax.experimental import pallas as pl
from jax.experimental.pallas import tpu as pltpu
from jax.sharding import PartitionSpec as P

FRAME = 2048
HOP = FRAME // 2
SMOOTH = 64
RIM = 8
STEPS = 2
NSRC = 8
LANES = 128
SCALE = RIM * (RIM + 1)
GROUPS = HOP // (2 * LANES)
VMEM = 14 * 1024 * 1024
SPLIT = 2
PIECES = 3
BF = jnp.bfloat16
F32 = jnp.float32


def tables():
    n = np.arange(HOP)
    lane = np.arange(LANES)
    theta = 2.0 * np.pi / FRAME
    first = np.array([2 * LANES * (i // 2) + i % 2 for i in range(2 * GROUPS)])
    steps = np.concatenate([2 * lane, first])

    def circle(rows):
        angle = theta * ((rows[:, None] * steps[None, :]) % FRAME)
        both = np.zeros((len(rows), 4 * LANES), np.float32)
        width = len(steps)
        both[:, :width] = np.cos(angle)
        both[:, 2 * LANES : 2 * LANES + width] = -np.sin(angle)
        return jnp.asarray(both)

    k = np.concatenate([np.arange(0, HOP, 2), np.arange(1, HOP, 2)])
    count = np.minimum(k + SMOOTH, HOP - 1) - np.maximum(k - SMOOTH, 0) + 1
    window = (0.5 - 0.5 * np.cos(theta * n))[None, :].astype(np.float32)
    i = np.arange(2 * LANES)
    src = np.where(i % 2 == 0, i // 2, LANES + i // 2)
    weave = (i[:, None] == src[None, :]).astype(np.float32)
    te, to, band = make_tables(circle(lane), circle(LANES * np.arange(HOP // LANES)))
    icount = jnp.asarray((1.0 / count)[None, :].astype(np.float32))
    return [te, to, band, icount, jnp.asarray(window), jnp.asarray(weave, BF)]


def tables_kernel(near_ref, far_ref, te_ref, to_ref, band_ref):
    rows = near_ref.shape[0]
    far = far_ref[pl.ds(pl.program_id(0), 1), :]

    def turned(lo):
        ar, ai = near_ref[:, lo : lo + LANES], near_ref[:, 2 * LANES + lo : 3 * LANES + lo]
        br, bi = far[:, lo : lo + LANES], far[:, 2 * LANES + lo : 3 * LANES + lo]
        return ar * br - ai * bi, ar * bi + ai * br

    re, im = turned(0)
    sr, si = turned(LANES)
    for i in range(2 * GROUPS):
        cr = sr[:, i : i + 1]
        ci = si[:, i : i + 1]
        ref = (te_ref, to_ref)[i % 2]
        lo = i // 2 * 2 * LANES
        ref[:, lo : lo + LANES] = (re * cr - im * ci).astype(BF)
        ref[:, lo + LANES : lo + 2 * LANES] = (re * ci + im * cr).astype(BF)
    half = HOP // 2

    def bin_of(i):
        return jnp.where(i < half, 2 * i, 2 * (i - half) + 1)

    r = bin_of(pl.program_id(0) * rows + lax.broadcasted_iota(jnp.int32, (rows, 1), 0))
    c = bin_of(lax.broadcasted_iota(jnp.int32, (1, HOP), 1))
    band_ref[...] = jnp.where(jnp.abs(r - c) <= SMOOTH, 1.0, 0.0).astype(BF)


def make_tables(near, far):
    rows = near.shape[0]
    shape = jax.ShapeDtypeStruct((HOP, HOP), BF)
    spec = pl.BlockSpec((rows, HOP), lambda i: (i, 0))
    return pl.pallas_call(
        tables_kernel,
        name="tables",
        grid=(HOP // rows,),
        in_specs=[pl.BlockSpec(x.shape, lambda i: (0, 0)) for x in (near, far)],
        out_specs=[spec] * 3,
        out_shape=[shape] * 3,
        compiler_params=pltpu.CompilerParams(vmem_limit_bytes=VMEM),
    )(near, far)


def tap(distance):
    d = jnp.abs(distance)
    return jnp.where(d == 0, float(SCALE), jnp.where(d <= RIM, (d - RIM - 1).astype(F32), 0.0))


def partial_kernel(me_ref, pos_ref, live_ref, x_ref, give_ref, keep_ref, low_ref, high_ref):
    channels, quarter = x_ref.shape
    here = me_ref[0] * channels + lax.broadcasted_iota(jnp.int32, (1, channels), 1)
    dist = pos_ref[...] - here
    live = live_ref[:1, :channels]
    taps = (tap(dist) * live).astype(BF)
    flag = jnp.sum(jnp.where(dist == 0, live, 0.0), axis=1, keepdims=True)
    part = jnp.dot(taps, x_ref[...], preferred_element_type=F32) * (1.0 / SCALE)
    part = part.astype(BF)
    tail = jnp.broadcast_to(flag, (flag.shape[0], LANES)).astype(BF)

    def put(ref):
        for step in range(STEPS):
            rows = slice(step * NSRC, (step + 1) * NSRC)
            ref[step, 0, :, :quarter] = part[rows]
            ref[step, 0, :, quarter:] = tail[rows]

    @pl.when(pl.program_id(0) < 2)
    def _():
        put(give_ref)

    @pl.when(pl.program_id(0) >= 2)
    def _():
        put(keep_ref)

    shape = (channels, channels)
    diagonal = lax.broadcasted_iota(jnp.int32, shape, 0) == lax.broadcasted_iota(jnp.int32, shape, 1)
    livec = jnp.sum(jnp.where(diagonal, live, 0.0), axis=1, keepdims=True)
    low_ref[...] = (x_ref[:RIM].astype(F32) * livec[:RIM]).astype(BF)
    high_ref[...] = (x_ref[channels - RIM :].astype(F32) * livec[channels - RIM :]).astype(BF)


def partial_sources(traces, live, pos, me):
    channels, samples = traces.shape
    quarter = samples // 4

    def place(i, me_ref):
        c = me_ref[0] & 1
        y = (me_ref[0] >> SPLIT) & 1
        half = jnp.where(i < 2, 1 - c, c)
        return 2 * half + jnp.where(i % 2 == 0, 1 - y, y)

    const = lambda i, me_ref: (0, 0)
    slab = jax.ShapeDtypeStruct((STEPS, 2, NSRC, quarter + LANES), BF)
    rim = jax.ShapeDtypeStruct((RIM, samples), BF)
    rim_spec = pl.BlockSpec((RIM, quarter), lambda i, me_ref: (0, place(i, me_ref)))
    return pl.pallas_call(
        partial_kernel,
        name="partial_sources",
        grid_spec=pltpu.PrefetchScalarGridSpec(
            num_scalar_prefetch=1,
            grid=(4,),
            in_specs=[
                pl.BlockSpec(pos.shape, const),
                pl.BlockSpec(live.shape, const),
                pl.BlockSpec((channels, quarter), lambda i, me_ref: (0, place(i, me_ref))),
            ],
            out_specs=[
                pl.BlockSpec((STEPS, 1, NSRC, quarter + LANES), lambda i, me_ref: (0, jnp.minimum(i, 1), 0, 0)),
                pl.BlockSpec((STEPS, 1, NSRC, quarter + LANES), lambda i, me_ref: (0, jnp.maximum(i - 2, 0), 0, 0)),
                rim_spec,
                rim_spec,
            ],
        ),
        out_shape=[slab, slab, rim, rim],
        compiler_params=pltpu.CompilerParams(vmem_limit_bytes=VMEM),
    )(me, pos, live, traces)


TABLE = pl.BlockSpec(memory_space=pltpu.VMEM)


def whiten_block(u, v, te_ref, to_ref, band_ref, ic_ref, store):
    y = [
        jnp.dot(u, te_ref[...], preferred_element_type=F32),
        jnp.dot(v, to_ref[...], preferred_element_type=F32),
    ]
    half = HOP // 2
    smooth = None
    for parity in range(2):
        power = []
        for g in range(GROUPS):
            re = y[parity][:, 2 * g * LANES : (2 * g + 1) * LANES]
            im = y[parity][:, (2 * g + 1) * LANES : (2 * g + 2) * LANES]
            power.append((re * re + im * im).astype(BF))
        power = jnp.concatenate(power, axis=1)
        part = jnp.dot(power, band_ref[parity * half : (parity + 1) * half], preferred_element_type=F32)
        smooth = part if smooth is None else smooth + part
    for parity in range(2):
        for g in range(GROUPS):
            lo = (parity * GROUPS + g) * LANES
            factor = lax.rsqrt(smooth[:, lo : lo + LANES] * ic_ref[:, lo : lo + LANES] + 1e-06)
            re = y[parity][:, 2 * g * LANES : (2 * g + 1) * LANES]
            im = y[parity][:, (2 * g + 1) * LANES : (2 * g + 2) * LANES]
            store(g, parity, *((x * factor).astype(BF).astype(F32) for x in (re, im)))


def own_kernel(pieces, channels, rows, live_ref, *refs):
    xs = refs[: 2 * pieces]
    te_ref, to_ref, band_ref, ic_ref, w_ref, out_ref, u_ref, v_ref = refs[2 * pieces :]
    frames = xs[0].shape[1] // HOP
    w = w_ref[...]
    width = sum(r.shape[0] for r in xs[:pieces])
    o = lax.broadcasted_iota(jnp.int32, (rows, 1), 0)
    i = lax.broadcasted_iota(jnp.int32, (1, width), 1)
    if pieces == 1:
        o = o + RIM
        live = live_ref[:1, :width]
    else:
        tail = channels - 2 * RIM
        o = jnp.where(o < RIM, o, o + tail)
        both = live_ref[...]
        lane = lax.broadcasted_iota(jnp.int32, both.shape, 1)
        back = pltpu.roll(both, LANES - tail + 2 * RIM, 1)
        both = jnp.where(lane < 2 * RIM, both, jnp.where(lane < 4 * RIM, back, 1.0))
        live = both[:1, :width]
        far = jnp.where(i < 5 * RIM, i - 5 * RIM, i - 5 * RIM + channels)
        i = jnp.where(i < 2 * RIM, i, jnp.where(i < 4 * RIM, i + tail - 2 * RIM, far))
    keep = jnp.sum(jnp.where(o == i, live, 0.0), axis=1, keepdims=True)
    a = (tap(o - i) * live * keep).astype(BF)

    def filt(f):
        if f < frames:
            parts = [r[:, f * HOP : (f + 1) * HOP] for r in xs[:pieces]]
        else:
            parts = [r[...] for r in xs[pieces:]]
        block = parts[0] if pieces == 1 else jnp.concatenate(parts, axis=0)
        full = jnp.dot(a, block, preferred_element_type=F32) * (1.0 / SCALE)
        return full.astype(BF).astype(F32)

    b = filt(0)
    early = b * w
    for f in range(frames):
        nb = filt(f + 1)
        nearly = nb * w
        late = nb - nearly
        u_ref[f * rows : (f + 1) * rows] = (early + late).astype(BF)
        v_ref[f * rows : (f + 1) * rows] = (early - late).astype(BF)
        early = nearly

    def store(g, parity, re, im):
        at = (2 * g + parity) * 3 * LANES
        for i, value in enumerate((re, re + im, im - re)):
            out_ref[:, :, at + i * LANES : at + (i + 1) * LANES] = value.reshape(frames, rows, LANES)

    whiten_block(u_ref[...], v_ref[...], te_ref, to_ref, band_ref, ic_ref, store)


def whiten_own(xs, live, rows, channels, tabs, per, first, frames):
    te, to, band, icount, window, _ = tabs
    j0 = first // per
    specs = [pl.BlockSpec((size, per * HOP), lambda j, b=at: (b, j0 + j)) for _, size, at in xs]
    specs += [pl.BlockSpec((size, HOP), lambda j, b=at: (b, (j0 + j + 1) * per)) for _, size, at in xs]
    return pl.pallas_call(
        functools.partial(own_kernel, len(xs), channels, rows),
        grid=(frames // per,),
        in_specs=[pl.BlockSpec(live.shape, lambda j: (0, 0))] + specs + [TABLE] * 5,
        out_specs=pl.BlockSpec((per, rows, 3 * HOP), lambda j: (j, 0, 0)),
        out_shape=jax.ShapeDtypeStruct((frames, rows, 3 * HOP), F32),
        scratch_shapes=[pltpu.VMEM((per * rows, HOP), BF), pltpu.VMEM((per * rows, HOP), BF)],
        compiler_params=pltpu.CompilerParams(vmem_limit_bytes=VMEM),
    )(live, *[x[0] for x in xs], *[x[0] for x in xs], te, to, band, icount, window)


def source_kernel(me_ref, mine_ref, twin_ref, pair_ref, far_ref, te_ref, to_ref, band_ref, ic_ref, w_ref, out_ref, x_ref, u_ref, v_ref):
    quarter = mine_ref.shape[2] - LANES
    rows = mine_ref.shape[1]
    frames = out_ref.shape[0]
    q = (me_ref[0] & 1) * 2 + ((me_ref[0] >> SPLIT) & 1)
    for at in range(4):

        @pl.when(q == at)
        def _(at=at):
            for flip, ref in ((0, mine_ref), (1, twin_ref), (2, pair_ref), (3, far_ref)):
                to = at ^ flip
                x_ref[:, to * quarter : (to + 1) * quarter] = ref[0, :, :quarter]

    flag = mine_ref[0, :, quarter:].astype(F32)[:, :1]
    w = w_ref[...]
    b = x_ref[:, :HOP].astype(F32) * flag
    early = b * w
    for f in range(0, frames, 2):
        us = []
        vs = []
        for g in (f, f + 1):
            nb = x_ref[:, (g + 1) * HOP : (g + 2) * HOP].astype(F32) * flag
            nearly = nb * w
            late = nb - nearly
            us.append(early + late)
            vs.append(early - late)
            early = nearly
        u_ref[f * rows : (f + 2) * rows] = jnp.concatenate(us, axis=0).astype(BF)
        v_ref[f * rows : (f + 2) * rows] = jnp.concatenate(vs, axis=0).astype(BF)

    def store(g, parity, re, im):
        at = (2 * g + parity) * 3 * LANES
        for i, value in enumerate((re, im, re + im)):
            out_ref[:, :, at + i * LANES : at + (i + 1) * LANES] = value.reshape(frames, rows, LANES)

    whiten_block(u_ref[...], v_ref[...], te_ref, to_ref, band_ref, ic_ref, store)


def whiten_source(me, quarters, tabs):
    te, to, band, icount, window, _ = tabs
    samples = 4 * (quarters[0].shape[2] - LANES)
    rows = quarters[0].shape[1]
    frames = samples // HOP - 1
    return pl.pallas_call(
        source_kernel,
        name="whiten_source",
        in_specs=[pl.BlockSpec(memory_space=pltpu.SMEM)] + [TABLE] * 9,
        out_specs=TABLE,
        out_shape=jax.ShapeDtypeStruct((frames, rows, 3 * HOP), F32),
        scratch_shapes=[
            pltpu.VMEM((rows, samples), BF),
            pltpu.VMEM((frames * rows, HOP), BF),
            pltpu.VMEM((frames * rows, HOP), BF),
        ],
        compiler_params=pltpu.CompilerParams(vmem_limit_bytes=VMEM),
    )(me, *quarters, te, to, band, icount, window)


SGRP = 4
UNROLL = 16


def cross_kernel(pieces, first, src_ref, *rest):
    mids = rest[: pieces[0]]
    edges = rest[pieces[0] : sum(pieces)]
    weave_ref = rest[sum(pieces)]
    out_ref, e_ref, im_ref = rest[-3:]
    frames, nsrc = src_ref.shape[:2]
    mid = mids[0].shape[1]
    edge = edges[0].shape[1]
    weave = weave_ref[...]
    group = pl.program_id(0) + first

    def product(refs, c0, parity, s0):
        lo = pl.multiple_of((2 * group + parity) * (3 * LANES), LANES)
        zero = jnp.zeros((16, LANES), F32)
        acc = tuple((zero, zero, zero) for _ in range(SGRP))
        start = 0
        for ref in refs:

            def body(f, acc, ref=ref, start=start):
                wr, ws, wd = (ref[f, pl.ds(c0, 16), pl.ds(lo + i * LANES, LANES)] for i in range(3))
                new = []
                for j in range(SGRP):
                    s = slice(s0 + j, s0 + j + 1)
                    sr, si, ss = (src_ref[start + f, s, pl.ds(lo + i * LANES, LANES)] for i in range(3))
                    a, b, c = acc[j]
                    new.append((a + sr * ws, b + ss * wr, c + si * wd))
                return tuple(new)

            acc = lax.fori_loop(0, ref.shape[0], body, acc, unroll=UNROLL)
            start += ref.shape[0]
        return [((b + c) * (1.0 / frames), (a - b) * (1.0 / frames)) for a, b, c in acc]

    @pl.when(pl.program_id(1) == 0)
    def _():
        rim = edge // 2

        def block(refs, spots, i):
            parity = i % 2
            c0 = pl.multiple_of(i // 2 * 16, 16)
            lane = pl.ds(pl.multiple_of(parity * LANES, LANES), LANES)
            for s0 in range(0, nsrc, SGRP):
                for j, both in enumerate(product(refs, c0, parity, s0)):
                    for part in range(2):
                        for to, a, b in spots:
                            e_ref[part, s0 + j, pl.ds(pl.multiple_of(to + c0, RIM), b - a), lane] = both[part][a:b]

        lax.fori_loop(0, mid // 8, lambda i, n: block(mids, ((rim, 0, 16),), i) or n, 0)
        lax.fori_loop(0, 2, lambda i, n: block(edges, ((0, 0, rim), (rim + mid, rim, 2 * rim)), i) or n, 0)

        for part in range(2):
            full = e_ref[part].reshape(nsrc * (mid + edge), 2 * LANES)
            hi = full.astype(BF)
            lo = (full - hi.astype(F32)).astype(BF)
            res = jnp.dot(hi, weave, preferred_element_type=F32) + jnp.dot(lo, weave, preferred_element_type=F32)
            res = res.reshape(nsrc, mid + edge, 2 * LANES)
            if part == 0:
                out_ref[0] = res
            else:
                im_ref[...] = res

    @pl.when(pl.program_id(1) != 0)
    def _():
        out_ref[0] = im_ref[...]


def cross(src, mids, edges, weave, step, first, groups, previous):
    _, nsrc, _ = src.shape
    channels = mids[0].shape[1] + edges[0].shape[1]
    shape = jax.ShapeDtypeStruct((STEPS, nsrc, channels, FRAME), F32)
    args = [src, *mids, *edges, weave]
    specs = [TABLE] * len(args)
    alias = {}
    if previous is not None:
        alias = {len(args): 0}
        args.append(previous)
        specs.append(pl.BlockSpec(memory_space=pl.ANY))
    return pl.pallas_call(
        functools.partial(cross_kernel, (len(mids), len(edges)), first),
        name="cross",
        grid=(groups, 2),
        in_specs=specs,
        out_specs=pl.BlockSpec((1, nsrc, channels, 2 * LANES), lambda g, p: (step, 0, 0, p * GROUPS + first + g)),
        out_shape=shape,
        scratch_shapes=[
            pltpu.VMEM((2, nsrc, channels, 2 * LANES), F32),
            pltpu.VMEM((nsrc, channels, 2 * LANES), F32),
        ],
        input_output_aliases=alias,
        compiler_params=pltpu.CompilerParams(vmem_limit_bytes=VMEM),
    )(*args)


def swap(block, bit):
    return lax.ppermute(block, "fiber", [(i, i ^ bit) for i in range(lax.axis_size("fiber"))])


def after(x, *deps):
    return lax.optimization_barrier((x, deps))[0]


def on_device(traces, live_mask, source_channels, source_owner):
    tabs = tables()
    channels, samples = traces.shape
    frames = samples // HOP - 1
    count = lax.axis_size("fiber")
    me = lax.axis_index("fiber").reshape(1)
    live = jnp.broadcast_to(jnp.pad(live_mask.astype(F32), (0, LANES - channels)), (8, LANES))

    pos = (source_owner[:, None] * channels + source_channels).reshape(STEPS * NSRC, 1)
    give, keep, low, high = partial_sources(traces, live, pos, me)

    span = frames // PIECES

    def mid(p, n, *deps):
        xs = [(traces, channels, 0)]
        return whiten_own(xs, after(live, *deps), channels - 2 * RIM, channels, tabs, 8, p * span, n * span)

    last = channels // (2 * RIM) - 1

    def edge(p, n, low, high, *deps):
        xs = [(traces, 2 * RIM, 0), (traces, 2 * RIM, last), (low, RIM, 0), (high, RIM, 0)]
        return whiten_own(xs, after(live, *deps), 2 * RIM, channels, tabs, 16, p * span, n * span)

    others = [1 << b for b in range(count.bit_length() - 2, 0, -1) if b != SPLIT]

    first = [swap(give[step], 1) for step in range(STEPS)]
    half_a = keep[0] + first[0]
    move = swap(half_a[:1], 1 << SPLIT)
    low_to, high_to = after((low, high), half_a)
    low = lax.ppermute(high_to, "fiber", [(i, i + 1) for i in range(count - 1)])
    high = lax.ppermute(low_to, "fiber", [(i + 1, i) for i in range(count - 1)])
    mids = [mid(0, 1, half_a)]
    piece_a = half_a[1:] + after(move, mids[0])
    move = swap(piece_a, others[0])
    half_b = keep[1] + after(first[1], piece_a)
    move_b = swap(half_b[:1], 1 << SPLIT)
    mids.append(mid(1, PIECES - 1, piece_a, half_b))
    piece_b = half_b[1:] + after(move_b, mids[1])
    for bit in others[1:]:
        piece_a = piece_a + after(move, mids[1])
        move = swap(piece_a, bit)
    move_b = swap(piece_b, others[0])
    edges = [edge(0, PIECES - 1, low, high, piece_a, piece_b)]
    piece_a = piece_a + after(move, edges[0])
    twin_a = swap(piece_a, 1 << SPLIT)
    pair_a = swap(piece_a, 1)
    edges.append(edge(PIECES - 1, 1, low, high, piece_a))
    for bit in others[1:]:
        piece_b = piece_b + after(move_b, edges[1])
        move_b = swap(piece_b, bit)
    far_a = swap(after(twin_a, edges[1]), 1)
    src = whiten_source(me, (piece_a, twin_a, pair_a, far_a), tabs)
    out = cross(src, mids, edges, tabs[5], 0, 0, 1, None)
    piece_b = piece_b + after(move_b, out)
    twin_b = swap(piece_b, 1 << SPLIT)
    pair_b = swap(piece_b, 1)
    out = cross(after(src, piece_b), mids, edges, tabs[5], 0, 1, 1, out)
    far_b = swap(after(twin_b, out), 1)
    out = cross(after(src, out, twin_b), mids, edges, tabs[5], 0, 2, GROUPS - 2, out)
    src = whiten_source(me, (piece_b, twin_b, pair_b, after(far_b, out)), tabs)
    out = cross(src, mids, edges, tabs[5], 1, 0, GROUPS, out)
    return out


def solution(mesh):
    placed = (P(("group", "fiber"), None), P(("group", "fiber")), P("group", None), P("group"))
    return jax.shard_map(
        on_device,
        mesh=mesh,
        in_specs=placed,
        out_specs=P(None, None, ("group", "fiber"), None),
        check_vma=False,
    )
```
